32 devices in a mesh: rep: 1, r: 8 (over y, z), s: 4 (over x, core).
Axes of the slice: x: 2, y: 2, z: 4, core: 2. Of those that a mesh axis runs over, the one named last changes fastest.
Arguments:
- x: bfloat16 [32, 4096, 640], P(('rep', 'r', 's'))
- dy: bfloat16 [32, 4096, 640], P(('rep', 'r', 's'))
- w_gate: bfloat16 [2, 640, 2432], P(None, 's')
- w_up: bfloat16 [2, 640, 2432], P(None, 's')
- w_down: bfloat16 [2, 2432, 640], P(None, 's')
- m_w_gate: float32 [2, 640, 2432], P(None, 's')
- m_w_up: float32 [2, 640, 2432], P(None, 's')
- m_w_down: float32 [2, 2432, 640], P(None, 's')
- v_w_gate: float32 [2, 640, 2432], P(None, 's')
- v_w_up: float32 [2, 640, 2432], P(None, 's')
- v_w_down: float32 [2, 2432, 640], P(None, 's')
Outputs:
- output 1: bfloat16 [2, 640, 2432], P('rep', 's')
- output 2: bfloat16 [2, 640, 2432], P('rep', 's')
- output 3: bfloat16 [2, 2432, 640], P('rep', 's')
- output 4: float32 [2, 640, 2432], P('rep', 's')
- output 5: float32 [2, 640, 2432], P('rep', 's')
- output 6: float32 [2, 2432, 640], P('rep', 's')
- output 7: float32 [2, 640, 2432], P('rep', 's')
- output 8: float32 [2, 640, 2432], P('rep', 's')
- output 9: float32 [2, 2432, 640], P('rep', 's')
All inputs are finite; a program needn't handle non-finite values.
Results may differ from the reference program's by a relative error of at most 0.022.
Values are sent between devices in bfloat16 or wider.
A program may use at most 2 GiB of HBM per device.

```python
import jax
import jax.numpy as jnp
from jax import lax

SEQUENCES = 32
TOKENS = 4096
D = 640
FF = 2432
LAYERS = 2
NAMES = ("w_gate", "w_up", "w_down")
SHAPES = {"w_gate": (LAYERS, D, FF), "w_up": (LAYERS, D, FF), "w_down": (LAYERS, FF, D)}


def bump(key, n, height):
    away = (jnp.arange(n, dtype=jnp.int32) - jax.random.randint(key, (), 0, n, jnp.int32)) % n
    return jnp.where(away < n // 8, height, 1.0)


def together(key, own, strength):
    shared = jax.random.normal(key, own.shape[1:], jnp.float32)
    return (own + strength * shared) * lax.rsqrt(1 + strength * strength)


def setup_inputs(seed: int = 0, part: int = 0) -> dict:
    kx, kdy, ka, kb, kz, kf, kh, kl, *keys = jax.random.split(jax.random.key(seed), 8 + 3 * len(NAMES))
    kx, kdy, ka, kb = (jax.random.fold_in(k, part) for k in (kx, kdy, ka, kb))
    kw, km, kv = (keys[i::3] for i in range(3))
    shape = (SEQUENCES, TOKENS, D)
    much_x, much_dy = jax.random.uniform(kz, (2,), jnp.float32, 0.0, 1.0)
    loud = 2.0 ** jax.random.uniform(jax.random.fold_in(kz, 1), (), jnp.float32, -1.0, 2.0)
    layers = 2.0 ** jax.random.uniform(kl, (LAYERS, 1, 1), jnp.float32, -1.0, 1.0)
    x = together(ka, jax.random.normal(kx, shape, jnp.float32), much_x) * bump(kf, D, 4.0)
    dy = together(kb, jax.random.normal(kdy, shape, jnp.float32), much_dy)
    drawn = {"x": x.astype(jnp.bfloat16), "dy": (loud * dy * (SEQUENCES * TOKENS) ** -0.5).astype(jnp.bfloat16)}
    for key, name in zip(kw, NAMES, strict=True):
        w = jax.random.normal(key, SHAPES[name], jnp.float32) * SHAPES[name][1] ** -0.5
        drawn[name] = (w * {"w_gate": 1.0, "w_up": bump(kh, FF, 4.0), "w_down": layers}[name]).astype(jnp.bfloat16)
    for key, name in zip(km, NAMES, strict=True):
        drawn[f"m_{name}"] = 0.1 * jax.random.normal(key, SHAPES[name], jnp.float32)
    for key, name in zip(kv, NAMES, strict=True):
        drawn[f"v_{name}"] = jax.random.uniform(key, SHAPES[name], jnp.float32, 0.005, 0.015)
    return drawn


def matmul(a, w):
    return jnp.dot(a, w, preferred_element_type=jnp.float32).astype(jnp.bfloat16)


def normed(h):
    wide = h.astype(jnp.float32)
    scale = lax.rsqrt(jnp.mean(wide**2, -1, keepdims=True) + 1e-6)
    return (wide * scale).astype(jnp.bfloat16)


def layer(h, w):
    a = normed(h)
    gate = jnp.dot(a, w["w_gate"], preferred_element_type=jnp.float32)
    up = jnp.dot(a, w["w_up"], preferred_element_type=jnp.float32)
    return h + matmul((jax.nn.silu(gate) * up).astype(jnp.bfloat16), w["w_down"])


def adamw(w, m, v, g):
    m = 0.9 * m + 0.1 * g
    v = 0.95 * v + 0.05 * g * g
    step = m * lax.rsqrt(v + 1e-8) + 0.1 * w
    return (w - 0.02 * step).astype(jnp.bfloat16), m, v


def clipped(gradients, sum_of_squares, count):
    factor = jnp.minimum(1.0, 0.5 * lax.rsqrt(sum_of_squares / count + 1e-30))
    return [g * factor for g in gradients]


def stack(weights, h):
    return lax.scan(lambda h, w: (layer(h, w), None), h, weights)[0]


def reference(x, dy, w_gate, w_up, w_down, m_w_gate, m_w_up, m_w_down, v_w_gate, v_w_up, v_w_down):
    weights = dict(zip(NAMES, (w_gate, w_up, w_down), strict=True))

    def take(so_far, sequence):
        h, by_y = sequence
        _, back = jax.vjp(lambda w: stack(w, h), weights)
        return jax.tree.map(lambda total, term: total + term.astype(jnp.float32), so_far, back(by_y)[0]), None

    none_yet = {name: jnp.zeros(w.shape, jnp.float32) for name, w in weights.items()}
    by_weights, _ = lax.scan(take, none_yet, (x, dy))
    gradients = [by_weights[name].astype(jnp.bfloat16).astype(jnp.float32) for name in NAMES]
    gradients = clipped(gradients, sum(jnp.sum(g * g) for g in gradients), sum(g.size for g in gradients))
    new = [
        adamw(w.astype(jnp.float32), m, v, g)
        for w, m, v, g in zip((w_gate, w_up, w_down), (m_w_gate, m_w_up, m_w_down), (v_w_gate, v_w_up, v_w_down), gradients, strict=True)
    ]
    return tuple(one[which] for which in range(3) for one in new)
```

```python
import functools

import jax
import jax.numpy as jnp
from jax import lax
from jax.experimental import pallas as pl
from jax.experimental.pallas import tpu as pltpu
from jax.sharding import PartitionSpec as P

F32, BF16 = jnp.float32, jnp.bfloat16
TILE = 512
VMEM_LIMIT = 62 * 1024 * 1024


def dot(a, b, ca=1, cb=0):
    return lax.dot_general(a, b, (((ca,), (cb,)), ((), ())), preferred_element_type=F32)


def cuts(n, size=256):
    return [(i, min(size, n - i)) for i in range(0, n, size)]


def params(*semantics):
    return pltpu.CompilerParams(dimension_semantics=semantics, vmem_limit_bytes=VMEM_LIMIT)


def rows(tile, width):
    return pl.BlockSpec((tile, width), lambda i: (i, 0))


def whole(*shape):
    return pl.BlockSpec(shape, lambda i: (0,) * len(shape))


def sds(shape, dtype):
    return jax.ShapeDtypeStruct(shape, dtype)


def cost(flops, nbytes):
    return pl.CostEstimate(flops=int(flops), bytes_accessed=int(nbytes), transcendentals=0)


def norm_of(h):
    wide = h.astype(F32)
    scale = lax.rsqrt(jnp.mean(wide * wide, -1, keepdims=True) + 1e-6)
    return (wide * scale).astype(BF16)


def silu_parts(g):
    sig = jax.nn.sigmoid(g)
    return sig, g * sig


def once(*shape):
    return pl.BlockSpec(shape, lambda i: (0,) * len(shape), pipeline_mode=pl.Buffered(1))


ANY = pl.BlockSpec(memory_space=pl.ANY)
MESH = pl.DeviceIdType.MESH
DMA = pltpu.SemaphoreType.DMA
ZS = 4


class Place:
    def __init__(self):
        r, s = lax.axis_index("r"), lax.axis_index("s")
        self.y, z, self.x, self.c = r // ZS, r % ZS, s // 2, s % 2
        self.za = ((z + 1) // 2) % 2
        self.ids = {
            "c": (0, r, 2 * self.x + 1 - self.c),
            "x": (0, r, 2 * (1 - self.x) + self.c),
            "y": (0, (1 - self.y) * ZS + z, s),
            "za": (0, self.y * ZS + z + 1 - 2 * (z % 2), s),
            "zb": (0, self.y * ZS + ZS - 1 - z, s),
        }

    def greet(self, names):
        barrier = pltpu.get_barrier_semaphore()
        for name in names:
            pl.semaphore_signal(barrier, inc=1, device_id=self.ids[name], device_id_type=MESH)
        pl.semaphore_wait(barrier, len(names))

    def copy(self, src, dst, send, recv, to):
        return pltpu.make_async_remote_copy(
            src_ref=src, dst_ref=dst, send_sem=send, recv_sem=recv, device_id=self.ids[to], device_id_type=MESH
        )


class Gather:
    def __init__(self, place, src, full, send, recv, local):
        n = src.shape[0]
        h = n // 2
        p = place
        own, far = 2 * p.x + p.c, 2 * (1 - p.x) + p.c

        def at(block, y, size):
            return full.at[pl.ds(pl.multiple_of(block * n + y * h, 16), size)]

        self.local = pltpu.make_async_copy(src, at(own, 0, n), local)
        self.x = p.copy(src.at[pl.ds(pl.multiple_of(p.y * h, 16), h)], at(own, p.y, h), send.at[0], recv.at[0], "x")
        self.y = p.copy(at(far, p.y, h), at(far, p.y, h), send.at[1], recv.at[1], "y")
        self.co = p.copy(src, at(own, 0, n), send.at[2], recv.at[2], "c")
        self.ca = p.copy(at(far, p.y, h), at(far, p.y, h), send.at[3], recv.at[3], "c")
        self.cb = p.copy(at(far, 1 - p.y, h), at(far, 1 - p.y, h), send.at[4], recv.at[4], "c")

    def start(self):
        self.x.start()
        self.co.start()
        self.local.start()

    def middle(self):
        self.x.wait_recv()
        self.y.start()
        self.ca.start()

    def last(self):
        self.y.wait_recv()
        self.cb.start()

    def finish(self):
        self.local.wait()
        for one in (self.co, self.ca, self.cb):
            one.wait_recv()
        for one in (self.x, self.y, self.co, self.ca, self.cb):
            one.wait_send()


def forward_body(x_ref, wg_ref, wu_ref, wd_ref, a_ref, g_ref, u_ref, h_ref, a1_ref, d0_ref, g1_ref, u1_ref, d1_ref, *scratch):
    fulls, (z_ref, send, recv, local) = scratch[:6], scratch[6:]
    i = pl.program_id(0)
    place = Place()
    blocks = [w.at[layer] for layer in range(2) for w in (wg_ref, wu_ref, wd_ref)]
    gathers = [Gather(place, blocks[k], fulls[k], send.at[k], recv.at[k], local.at[k]) for k in range(6)]

    @pl.when(i == 0)
    def _():
        place.greet("cxy")
        for one in gathers[:3]:
            one.start()
        for one in gathers[:3]:
            one.middle()
        for one in gathers[:3]:
            one.last()
        for one in gathers[:3]:
            one.finish()
        for one in gathers[3:]:
            one.start()

    for k in range(3):

        @pl.when(i == 3 + 3 * k)
        def _(one=gathers[3 + k]):
            one.middle()

        @pl.when(i == 6 + 3 * k)
        def _(one=gathers[3 + k]):
            one.last()

    a = norm_of(x_ref[...])
    a_ref[...] = a
    for at, n in cuts(z_ref.shape[1]):
        at = slice(at, at + n)
        g = dot(a, fulls[0][:, at])
        u = dot(a, fulls[1][:, at])
        g_ref[:, at] = g
        u_ref[:, at] = u
        z_ref[:, at] = (silu_parts(g)[1] * u).astype(BF16)
    h = (x_ref[...].astype(F32) + dot(z_ref[...], fulls[2][...]).astype(BF16).astype(F32)).astype(BF16)
    h_ref[...] = h
    a1_ref[...] = norm_of(h)

    @pl.when(i == pl.num_programs(0) - 1)
    def _():
        for one in gathers[3:]:
            one.finish()
        outs = [pltpu.make_async_copy(fulls[2 + k], out, local.at[k]) for k, out in enumerate((d0_ref, g1_ref, u1_ref, d1_ref))]
        for one in outs:
            one.start()
        for one in outs:
            one.wait()


def forward(x, wg, wu, wd):
    t, d = x.shape
    f = wg.shape[2]
    tile = 256
    mats = [(d, f), (d, f), (f, d)] * 2
    return pl.pallas_call(
        forward_body,
        grid=(t // tile,),
        in_specs=[rows(tile, d), ANY, ANY, ANY],
        out_specs=[rows(tile, d), rows(tile, f), rows(tile, f), rows(tile, d), rows(tile, d)] + [ANY] * 4,
        out_shape=[sds((t, d), BF16), sds((t, f), F32), sds((t, f), F32), sds((t, d), BF16), sds((t, d), BF16)]
        + [sds(one, BF16) for one in mats[2:]],
        scratch_shapes=[pltpu.VMEM(one, BF16) for one in mats] + [pltpu.VMEM((tile, f), BF16), DMA((6, 5)), DMA((6, 5)), DMA((6,))],
        compiler_params=pltpu.CompilerParams(
            dimension_semantics=("arbitrary",), vmem_limit_bytes=VMEM_LIMIT, collective_id=0, has_side_effects=True
        ),
        cost_estimate=cost(6 * t * d * f, 12 * t * f),
        name="forward",
    )(x, wg, wu, wd)


class Sum:
    def __init__(self, place, term, out, squares, buffers, sems):
        self.p, self.term, self.out, self.squares = place, term, out, squares
        self.rc, self.rx, self.sx, self.keep, self.ry, self.ra, self.rb, self.fin, self.temp = buffers
        send, recv, self.local = sems
        p = place
        self.ka, self.kx = [], None
        for x in range(2):
            self.ka.append(p.copy(term.at[pl.ds(4 * (2 * x + 1 - p.c), 4)], self.rc.at[x], send.at[x], recv.at[x], "c"))
        self.cx = p.copy(self.sx, self.rx, send.at[2], recv.at[2], "x")
        two, one, last = self.sx.at[pl.ds(0, 2)], self.sx.at[2], self.sx.at[3]
        self.cy = p.copy(two, self.ry, send.at[3], recv.at[3], "y")
        self.cza = p.copy(one, self.ra, send.at[4], recv.at[4], "za")
        self.czb = p.copy(last, self.rb, send.at[5], recv.at[5], "zb")
        self.at = 2 * p.y + p.za
        mine = self.fin.at[self.at]
        self.back = p.copy(mine, mine, send.at[6], recv.at[6], "za")
        half = self.fin.at[pl.ds(2 * p.y, 2)]
        self.wide = p.copy(half, half, send.at[7], recv.at[7], "y")
        self.done = pltpu.make_async_copy(self.fin, out, self.local.at[0])

    def a(self):
        for one in self.ka:
            one.start()

    def b(self):
        p = self.p
        for one in self.ka:
            one.wait_recv()
        loads = []
        for k, x in enumerate((1 - p.x, p.x)):
            loads.append(pltpu.make_async_copy(self.term.at[pl.ds(4 * (2 * x + p.c), 4)], self.temp.at[2 * k], self.local.at[2 * k]))
            loads.append(pltpu.make_async_copy(self.rc.at[x], self.temp.at[2 * k + 1], self.local.at[2 * k + 1]))
        for one in loads:
            one.start()
        for one in loads[:2]:
            one.wait()
        for q in range(4):
            self.sx[q] = (self.temp[0, q].astype(F32) + self.temp[1, q].astype(F32)).astype(BF16)
        self.cx.start()
        for one in loads[2:]:
            one.wait()
        for q in range(4):
            self.keep[q] = self.temp[2, q].astype(F32) + self.temp[3, q].astype(F32)

    def c_(self):
        self.cx.wait()
        load = pltpu.make_async_copy(self.rx, self.temp.at[0], self.local.at[0])
        load.start()
        load.wait()
        p = self.p
        for q in range(2):
            at = 2 * (1 - p.y) + q
            self.sx[q] = (self.keep[at] + self.temp[0, at].astype(F32)).astype(BF16)
        self.cy.start()
        for q in range(2):
            at = 2 * p.y + q
            self.keep[at] = self.keep[at] + self.temp[0, at].astype(F32)

    def d(self):
        self.cy.wait_recv()
        p = self.p
        self.sx[2] = (self.keep[2 * p.y + 1 - p.za] + self.ry[1 - p.za].astype(F32)).astype(BF16)
        self.cza.start()
        self.keep[self.at] = self.keep[self.at] + self.ry[p.za].astype(F32)

    def e(self):
        self.cza.wait_recv()
        self.sx[3] = (self.keep[self.at] + self.ra[...].astype(F32)).astype(BF16)
        self.czb.start()

    def f(self):
        self.czb.wait_recv()
        piece = (self.sx[3].astype(F32) + self.rb[...].astype(F32)).astype(BF16)
        self.fin[self.at] = piece
        self.back.start()
        wide = piece.astype(F32)
        self.squares[0, 0] += jnp.sum(wide * wide)

    def g(self):
        self.back.wait_recv()
        self.wide.start()

    def h(self):
        self.wide.wait_recv()
        self.done.start()

    def finish(self):
        for one in self.ka + [self.cy, self.cza, self.czb, self.back, self.wide]:
            one.wait_send()
        self.done.wait()


def quarters(shape):
    return (16, shape[0] // 16, shape[1])


def sum_scratch(shape):
    _, a, b = shape
    return [
        pltpu.VMEM((4, a, b), BF16),
        pltpu.VMEM((4, a, b), F32),
        pltpu.VMEM((2, a, b), BF16),
        pltpu.VMEM((a, b), BF16),
        pltpu.VMEM((a, b), BF16),
        pltpu.VMEM((4, a, b), BF16),
    ]


def landing(shape):
    return [sds((2, 4) + shape[1:], BF16), sds((4,) + shape[1:], BF16)]


def kept_out(shape):
    return sds((4,) + shape[1:], BF16)


def split_up(at, per, refs, count=3):
    return [refs[at + k * per : at + (k + 1) * per] for k in range(count)]


def make_sums(place, terms, outs, squares, lands, own, temps, sems):
    send, recv, local = sems
    return [
        Sum(
            place,
            terms[k],
            outs[k],
            squares,
            (lands[k][0], lands[k][1], own[k][0], own[k][1], own[k][2], own[k][3], own[k][4], own[k][5], temps[terms[k].shape[2]]),
            (send.at[k], recv.at[k], local.at[k]),
        )
        for k in range(len(terms))
    ]


NEAR = ("c", "x", "y", "za", "zb")


def algebra(g, u, dz):
    sig, act = silu_parts(g)
    z = (act * u).astype(BF16)
    dz = dz.astype(BF16).astype(F32)
    du = (dz * act).astype(BF16)
    dg = (dz * u * (sig + act * (1.0 - sig))).astype(BF16)
    return z, dg, du


def store_turned(out, acc):
    n = out.shape[1]
    for at in range(0, acc.shape[1], 128):
        block = acc[:, at : at + 128].T.astype(BF16)
        row = at
        while row < at + 128:
            k, r = row // n, row % n
            more = min(n - r, at + 128 - row)
            out[k, r : r + more, :] = block[row - at : row - at + more, :]
            row += more


def store_quarters(out, acc):
    n = out.shape[1]
    for k in range(out.shape[0]):
        out[k] = acc[k * n : (k + 1) * n, :].astype(BF16)


def hidden_body(a_ref, dy_ref, wg_ref, wu_ref, wd_ref, dg_ref, du_ref, dwd_ref, acc):
    i = pl.program_id(0)

    @pl.when(i == 0)
    def _():
        acc[...] = jnp.zeros_like(acc)

    a, dy = a_ref[...], dy_ref[...]
    across = dy.T
    for at, n in cuts(acc.shape[1]):
        at = slice(at, at + n)
        g, u = dot(a, wg_ref[:, at]), dot(a, wu_ref[:, at])
        z, dg, du = algebra(g, u, dot(dy, wd_ref[at, :], 1, 1))
        dg_ref[:, at] = dg
        du_ref[:, at] = du
        acc[:, at] += dot(across, z)

    @pl.when(i == pl.num_programs(0) - 1)
    def _():
        store_turned(dwd_ref, acc)


def hidden(a, dy, wg, wu, wd):
    t, d = dy.shape
    f = wd.shape[0]
    tile = 512
    shape = quarters((f, d))
    return pl.pallas_call(
        hidden_body,
        grid=(t // tile,),
        in_specs=[rows(tile, d), rows(tile, d), once(d, f), once(d, f), once(f, d)],
        out_specs=[rows(tile, f), rows(tile, f), once(*shape)],
        out_shape=[sds((t, f), BF16), sds((t, f), BF16), sds(shape, BF16)],
        scratch_shapes=[pltpu.VMEM((d, f), F32)],
        compiler_params=params("arbitrary"),
        cost_estimate=cost(8 * t * d * f, 12 * t * f),
        name="hidden",
    )(a, dy, wg, wu, wd)


def grads_body(a_ref, c_ref, e_ref, out_c, out_e, acc_c, acc_e):
    i = pl.program_id(0)

    @pl.when(i == 0)
    def _():
        acc_c[...] = jnp.zeros_like(acc_c)
        acc_e[...] = jnp.zeros_like(acc_e)

    across = a_ref[...].T
    for acc, ref in ((acc_c, c_ref), (acc_e, e_ref)):
        for at, n in cuts(ref.shape[1]):
            at = slice(at, at + n)
            acc[:, at] += dot(across, ref[:, at])

    @pl.when(i == pl.num_programs(0) - 1)
    def _():
        store_quarters(out_c, acc_c)
        store_quarters(out_e, acc_e)


def grads(a, c, e):
    (t, d), f = a.shape, c.shape[1]
    tile = 512
    shape = quarters((d, f))
    return pl.pallas_call(
        grads_body,
        grid=(t // tile,),
        in_specs=[rows(tile, d), rows(tile, f), rows(tile, f)],
        out_specs=[once(*shape)] * 2,
        out_shape=[sds(shape, BF16)] * 2,
        scratch_shapes=[pltpu.VMEM((d, f), F32)] * 2,
        compiler_params=params("arbitrary"),
        cost_estimate=cost(4 * t * d * f, 4 * t * f),
        name="grads",
    )(a, c, e)


def back_body(dg1, du1, h_ref, dy_ref, g_ref, u_ref, wg_ref, wu_ref, wd_ref, *refs):
    terms, refs = refs[:3], refs[3:]
    dg_ref, du_ref, dwd_ref, sq_ref = refs[:4]
    outs, lands, refs = refs[4:7], [refs[7:9], refs[9:11], refs[11:13]], refs[13:]
    acc, own, refs = refs[0], split_up(1, 6, refs), refs[19:]
    temps = {terms[0].shape[2]: refs[0], terms[2].shape[2]: refs[1]}
    i = pl.program_id(0)
    place = Place()
    sums = make_sums(place, terms, outs, sq_ref, lands, own, temps, refs[2:5])

    @pl.when(i == 0)
    def _():
        place.greet(NEAR)
        sq_ref[0, 0] = 0.0
        for k in (2, 0, 1):
            sums[k].a()
        acc[...] = jnp.zeros_like(acc)

    plan = {1: ("b2", "b0", "b1"), 4: ("c2",), 6: ("d2", "c0"), 7: ("e2",), 8: ("d0", "f2", "c1"), 9: ("e0",), 10: ("g2", "d1", "f0"), 11: ("e1",), 12: ("h2", "g0", "f1"), 13: ("g1",), 14: ("h0",), 15: ("h1",)}
    for at, what in plan.items():

        @pl.when(i == at)
        def _(what=what):
            for one in what:
                stage(sums, one)

    da = dot(dg1[...], wg_ref[...], 1, 1) + dot(du1[...], wu_ref[...], 1, 1)
    da = da.astype(BF16).astype(F32)
    h = h_ref[...].astype(F32)
    count = h.shape[-1]
    scale = lax.rsqrt(jnp.sum(h * h, -1, keepdims=True) / count + 1e-6)
    inner = jnp.sum(da * h, -1, keepdims=True) / count
    dh = da * scale - h * (inner * (scale * scale * scale))
    dh = (dy_ref[...].astype(F32) + dh.astype(BF16).astype(F32)).astype(BF16)
    across = dh.T
    for at, n in cuts(acc.shape[1]):
        at = slice(at, at + n)
        z, dg, du = algebra(g_ref[:, at], u_ref[:, at], dot(dh, wd_ref[at, :], 1, 1))
        dg_ref[:, at] = dg
        du_ref[:, at] = du
        acc[:, at] += dot(across, z)

    @pl.when(i == pl.num_programs(0) - 1)
    def _():
        store_turned(dwd_ref, acc)
        for one in sums:
            one.finish()


def stage(sums, what):
    one = sums[int(what[1])]
    {"a": one.a, "b": one.b, "c": one.c_, "d": one.d, "e": one.e, "f": one.f, "g": one.g, "h": one.h}[what[0]]()


def sum_outs(shapes):
    kinds = [kept_out(one) for one in shapes]
    for one in shapes:
        kinds += landing(one)
    return kinds


def sum_own(shapes):
    out = []
    for one in shapes:
        out += sum_scratch(one)
    for one in dict.fromkeys(shapes):
        out.append(pltpu.VMEM((4, 4) + one[1:], BF16))
    n = len(shapes)
    return out + [DMA((n, 8)), DMA((n, 8)), DMA((n, 4))]


def back(dg1, du1, h, dy, g0, u0, wg, wu, wd, terms):
    t, d = h.shape
    f = wd.shape[0]
    tile = 256
    shapes = [one.shape for one in terms]
    out = quarters((f, d))
    kinds = sum_outs(shapes)
    results = pl.pallas_call(
        back_body,
        grid=(t // tile,),
        in_specs=[rows(tile, f), rows(tile, f), rows(tile, d), rows(tile, d), rows(tile, f), rows(tile, f)]
        + [once(d, f), once(d, f), once(f, d)]
        + [ANY] * 3,
        out_specs=[rows(tile, f), rows(tile, f), once(*out), pl.BlockSpec(memory_space=pltpu.SMEM)] + [ANY] * len(kinds),
        out_shape=[sds((t, f), BF16), sds((t, f), BF16), sds(out, BF16), sds((1, 1), F32)] + kinds,
        scratch_shapes=[pltpu.VMEM((d, f), F32)] + sum_own(shapes),
        compiler_params=pltpu.CompilerParams(
            dimension_semantics=("arbitrary",), vmem_limit_bytes=67043328, collective_id=1, has_side_effects=True
        ),
        cost_estimate=cost(8 * t * d * f, 12 * t * f),
        name="back",
    )(dg1, du1, h, dy, g0, u0, wg, wu, wd, *terms)
    return results[:3], results[3], results[4:7]


def tail_body(a_ref, c_ref, e_ref, term_d, sq1_ref, *refs):
    tot_ref, outs, lands, refs = refs[0], refs[1:5], split_up(5, 2, refs, 4), refs[13:]
    sq_ref, acc, made, own, refs = refs[0], refs[1], refs[2:5], split_up(5, 6, refs, 4), refs[29:]
    terms = (*made, term_d)
    temps = {one.shape[2]: refs[k] for k, one in enumerate(terms)}
    tot_in, tot_send, tot_recv = refs[7:10]
    i = pl.program_id(0)
    n = pl.num_programs(0) // 3
    cut = made[1].shape[2]
    place = Place()
    sums = make_sums(place, terms, outs, sq_ref, lands, own, temps, refs[4:7])

    @pl.when(i == 0)
    def _():
        place.greet(NEAR)
        sq_ref[0, 0] = sq1_ref[0, 0]
        sums[3].a()

    @pl.when((i == 0) | (i == n))
    def _():
        acc[...] = jnp.zeros_like(acc)

    plan = {1: ("b3",), 4: ("b0",), 5: ("c3",), 8: ("b1", "d3"), 9: ("c0", "e3"), 10: ("f3",), 11: ("g3", "d0")}
    for at, what in plan.items():

        @pl.when(i == at)
        def _(what=what):
            for one in what:
                stage(sums, one)

    def add(ref, lo, hi):
        across = a_ref[...].T
        for at in range(lo, hi, 256):
            at = slice(at, min(at + 256, hi))
            acc[:, at] += dot(across, ref[:, at])

    for k, (ref, lo, hi) in enumerate(((c_ref, 0, c_ref.shape[1]), (e_ref, 0, cut), (e_ref, cut, c_ref.shape[1]))):

        @pl.when((i >= k * n) & (i < (k + 1) * n))
        def _(ref=ref, lo=lo, hi=hi):
            add(ref, lo, hi)

        @pl.when(i == (k + 1) * n - 1)
        def _(k=k, lo=lo, hi=hi):
            rows_each = made[k].shape[1]
            for q in range(16):
                made[k][q] = acc[q * rows_each : (q + 1) * rows_each, lo:hi].astype(BF16)
            sums[k].a()

    @pl.when(i == pl.num_programs(0) - 1)
    def _():
        for one in ("b2", "e0", "c1", "h3", "f0", "d1", "c2", "g0", "e1", "d2", "f1", "e2", "g1", "f2"):
            stage(sums, one)
        tot_ref[...] = jnp.full(tot_ref.shape, sq_ref[0, 0], F32)
        for k, name in enumerate(("c", "x", "y", "za")):
            if k == 1:
                sums[2].g()
            one = place.copy(tot_ref, tot_in.at[k], tot_send.at[k], tot_recv.at[k], name)
            one.start()
            one.wait()
            tot_ref[...] = tot_ref[...] + tot_in[k]
        for one in ("h0", "h1", "h2"):
            stage(sums, one)
        for one in sums:
            one.finish()


def tail(a, c, e, term_d, squares):
    (t, d), f = a.shape, c.shape[1]
    tile = 1024
    n = t // tile
    cut = f // 256 // 2 * 256 + 256
    made = quarters((d, f))
    shapes = [made, made[:2] + (cut,), made[:2] + (f - cut,), term_d.shape]
    kinds = sum_outs(shapes)
    smem = pl.BlockSpec(memory_space=pltpu.SMEM)
    results = pl.pallas_call(
        tail_body,
        grid=(3 * n,),
        in_specs=[
            pl.BlockSpec((tile, d), lambda i: (i % n, 0)),
            pl.BlockSpec((tile, f), lambda i: (jnp.minimum(i, n - 1), 0)),
            pl.BlockSpec((tile, f), lambda i: (jnp.where(i < n, 0, i % n), 0)),
            ANY,
            smem,
        ],
        out_specs=[pl.BlockSpec((8, 128), lambda i: (0, 0))] + [ANY] * len(kinds),
        out_shape=[sds((8, 128), F32)] + kinds,
        scratch_shapes=[pltpu.SMEM((1, 1), F32), pltpu.VMEM((d, f), F32)]
        + [pltpu.VMEM(one, BF16) for one in shapes[:3]]
        + sum_own(shapes)
        + [pltpu.VMEM((4, 8, 128), F32), DMA((4,)), DMA((4,))],
        compiler_params=pltpu.CompilerParams(
            dimension_semantics=("arbitrary",), vmem_limit_bytes=67043328, collective_id=2, has_side_effects=True
        ),
        cost_estimate=cost(4 * t * d * f, 4 * t * f),
        name="tail",
    )(a, c, e, term_d, squares)
    return results[0][0, 0], results[1:5]


def solution(mesh):
    def step(x, dy, *arrays):
        x, dy = x[0], dy[0]
        weights, m, v = (arrays[i : i + 3] for i in (0, 3, 6))
        a0, g0, u0, h1, a1, wd0, wg1, wu1, wd1 = forward(x, *weights)
        dg1, du1, d_wd1 = hidden(a1, dy, wg1, wu1, wd1)
        d_wg1, d_wu1 = grads(a1, dg1, du1)
        (dg0, du0, d_wd0), squares1, sums1 = back(dg1, du1, h1, dy, g0, u0, wg1, wu1, wd0, (d_wg1, d_wu1, d_wd1))
        squares, (s_g, s_ua, s_ub, s_d) = tail(a0, dg0, du0, d_wd0, squares1)
        sums0 = (s_g, jnp.concatenate([s_ua, s_ub], -1), s_d)
        count = 4 * sum(w.size for w in weights)
        factor = jnp.minimum(1.0, 0.5 * lax.rsqrt(squares / count + 1e-30))
        new = []
        for i in range(3):
            g = jnp.stack([sums0[i], sums1[i]]).reshape(weights[i].shape).astype(F32) * factor
            w = weights[i].astype(F32)
            mi = 0.9 * m[i] + 0.1 * g
            vi = 0.95 * v[i] + 0.05 * g * g
            new.append(((w - 0.02 * (mi * lax.rsqrt(vi + 1e-8) + 0.1 * w)).astype(BF16), mi, vi))
        return tuple(one[which] for which in range(3) for one in new)

    states, cut = P(("rep", "r", "s"), None, None), P(None, "s", None)
    return jax.shard_map(
        step,
        mesh=mesh,
        in_specs=(states, states) + (cut,) * 9,
        out_specs=(P("rep", "s", None),) * 9,
        check_vma=False,
    )
```

```python
import functools

import jax
import jax.numpy as jnp
from jax import lax
from jax.experimental import pallas as pl
from jax.experimental.pallas import tpu as pltpu
from jax.sharding import PartitionSpec as P

F32, BF16 = jnp.float32, jnp.bfloat16
HIDDEN_TILE = 512
TILE = 512
VMEM_LIMIT = 62 * 1024 * 1024


def dot(a, b, ca=1, cb=0):
    return lax.dot_general(a, b, (((ca,), (cb,)), ((), ())), preferred_element_type=F32)


def cuts(n, size=256):
    return [(i, min(size, n - i)) for i in range(0, n, size)]


def params(*semantics):
    return pltpu.CompilerParams(dimension_semantics=semantics, vmem_limit_bytes=VMEM_LIMIT)


def rows(tile, width):
    return pl.BlockSpec((tile, width), lambda i: (i, 0))


def columns(height, tile):
    return pl.BlockSpec((height, tile), lambda i: (0, i))


def whole(*shape):
    return pl.BlockSpec(shape, lambda i: (0,) * len(shape))


def sds(shape, dtype):
    return jax.ShapeDtypeStruct(shape, dtype)


def cost(flops, nbytes):
    return pl.CostEstimate(flops=int(flops), bytes_accessed=int(nbytes), transcendentals=0)


def norm_of(h):
    wide = h.astype(F32)
    scale = lax.rsqrt(jnp.mean(wide * wide, -1, keepdims=True) + 1e-6)
    return (wide * scale).astype(BF16)


def silu_parts(g):
    sig = jax.nn.sigmoid(g)
    return sig, g * sig


def once(*shape):
    return pl.BlockSpec(shape, lambda i: (0,) * len(shape), pipeline_mode=pl.Buffered(1))


ANY = pl.BlockSpec(memory_space=pl.ANY)
MESH = pl.DeviceIdType.MESH
DMA = pltpu.SemaphoreType.DMA
ZS = 4


class Place:
    def __init__(self):
        r, s = lax.axis_index("r"), lax.axis_index("s")
        self.y, z, self.x, self.c = r // ZS, r % ZS, s // 2, s % 2
        self.za = ((z + 1) // 2) % 2
        self.ids = {
            "c": (0, r, 2 * self.x + 1 - self.c),
            "x": (0, r, 2 * (1 - self.x) + self.c),
            "y": (0, (1 - self.y) * ZS + z, s),
            "za": (0, self.y * ZS + z + 1 - 2 * (z % 2), s),
            "zb": (0, self.y * ZS + ZS - 1 - z, s),
        }

    def greet(self, names):
        barrier = pltpu.get_barrier_semaphore()
        for name in names:
            pl.semaphore_signal(barrier, inc=1, device_id=self.ids[name], device_id_type=MESH)
        pl.semaphore_wait(barrier, len(names))

    def copy(self, src, dst, send, recv, to):
        return pltpu.make_async_remote_copy(
            src_ref=src, dst_ref=dst, send_sem=send, recv_sem=recv, device_id=self.ids[to], device_id_type=MESH
        )


class Gather:
    def __init__(self, place, src, full, send, recv, local):
        n = src.shape[0]
        h = n // 2
        p = place
        own, far = 2 * p.x + p.c, 2 * (1 - p.x) + p.c

        def at(block, y, size):
            return full.at[pl.ds(pl.multiple_of(block * n + y * h, 16), size)]

        self.local = pltpu.make_async_copy(src, at(own, 0, n), local)
        self.x = p.copy(src.at[pl.ds(pl.multiple_of(p.y * h, 16), h)], at(own, p.y, h), send.at[0], recv.at[0], "x")
        self.y = p.copy(at(far, p.y, h), at(far, p.y, h), send.at[1], recv.at[1], "y")
        self.co = p.copy(src, at(own, 0, n), send.at[2], recv.at[2], "c")
        self.ca = p.copy(at(far, p.y, h), at(far, p.y, h), send.at[3], recv.at[3], "c")
        self.cb = p.copy(at(far, 1 - p.y, h), at(far, 1 - p.y, h), send.at[4], recv.at[4], "c")

    def start(self):
        self.x.start()
        self.co.start()
        self.local.start()

    def middle(self):
        self.x.wait_recv()
        self.y.start()
        self.ca.start()

    def last(self):
        self.y.wait_recv()
        self.cb.start()

    def finish(self):
        self.local.wait()
        for one in (self.co, self.ca, self.cb):
            one.wait_recv()
        for one in (self.x, self.y, self.co, self.ca, self.cb):
            one.wait_send()


def forward_body(x_ref, wg_ref, wu_ref, wd_ref, g_ref, u_ref, h_ref, a1_ref, across_ref, across1_ref, d0_ref, g1_ref, u1_ref, d1_ref, *scratch):
    fulls, (z_ref, send, recv, local) = scratch[:6], scratch[6:]
    i = pl.program_id(0)
    place = Place()
    blocks = [w.at[layer] for layer in range(2) for w in (wg_ref, wu_ref, wd_ref)]
    gathers = [Gather(place, blocks[k], fulls[k], send.at[k], recv.at[k], local.at[k]) for k in range(6)]

    @pl.when(i == 0)
    def _():
        place.greet("cxy")
        for one in gathers[:3]:
            one.start()
        for one in gathers[:3]:
            one.middle()
        for one in gathers[:3]:
            one.last()
        for one in gathers[:3]:
            one.finish()
        for one in gathers[3:]:
            one.start()

    for k in range(3):

        @pl.when(i == 3 + 3 * k)
        def _(one=gathers[3 + k]):
            one.middle()

        @pl.when(i == 6 + 3 * k)
        def _(one=gathers[3 + k]):
            one.last()

    a = norm_of(x_ref[...])
    across_ref[...] = a.T
    for at, n in cuts(z_ref.shape[1]):
        at = slice(at, at + n)
        g = dot(a, fulls[0][:, at])
        u = dot(a, fulls[1][:, at])
        g_ref[:, at] = g
        u_ref[:, at] = u
        z_ref[:, at] = (silu_parts(g)[1] * u).astype(BF16)
    h = (x_ref[...].astype(F32) + dot(z_ref[...], fulls[2][...]).astype(BF16).astype(F32)).astype(BF16)
    h_ref[...] = h
    a1 = norm_of(h)
    a1_ref[...] = a1
    across1_ref[...] = a1.T

    @pl.when(i == pl.num_programs(0) - 1)
    def _():
        for one in gathers[3:]:
            one.finish()
        outs = [pltpu.make_async_copy(fulls[2 + k], out, local.at[k]) for k, out in enumerate((d0_ref, g1_ref, u1_ref, d1_ref))]
        for one in outs:
            one.start()
        for one in outs:
            one.wait()


def forward(x, wg, wu, wd):
    t, d = x.shape
    f = wg.shape[2]
    tile = 256
    mats = [(d, f), (d, f), (f, d)] * 2
    return pl.pallas_call(
        forward_body,
        grid=(t // tile,),
        in_specs=[rows(tile, d), ANY, ANY, ANY],
        out_specs=[rows(tile, f), rows(tile, f), rows(tile, d), rows(tile, d), columns(d, tile), columns(d, tile)] + [ANY] * 4,
        out_shape=[sds((t, f), F32), sds((t, f), F32), sds((t, d), BF16), sds((t, d), BF16), sds((d, t), BF16), sds((d, t), BF16)]
        + [sds(one, BF16) for one in mats[2:]],
        scratch_shapes=[pltpu.VMEM(one, BF16) for one in mats] + [pltpu.VMEM((tile, f), BF16), DMA((6, 5)), DMA((6, 5)), DMA((6,))],
        compiler_params=pltpu.CompilerParams(
            dimension_semantics=("arbitrary",), vmem_limit_bytes=VMEM_LIMIT, collective_id=0, has_side_effects=True
        ),
        cost_estimate=cost(6 * t * d * f, 12 * t * f),
        name="forward",
    )(x, wg, wu, wd)


class Sum:
    def __init__(self, place, term, out, squares, buffers, sems):
        self.p, self.term, self.out, self.squares = place, term, out, squares
        self.rc, self.rx, self.sx, self.keep, self.ry, self.ra, self.rb, self.fin = buffers
        send, recv, self.local = sems
        p = place
        self.ka, self.kx = [], None
        for x in range(2):
            self.ka.append(p.copy(term.at[pl.ds(4 * (2 * x + 1 - p.c), 4)], self.rc.at[x], send.at[x], recv.at[x], "c"))
        self.cx = p.copy(self.sx, self.rx, send.at[2], recv.at[2], "x")
        two, one, last = self.sx.at[pl.ds(0, 2)], self.sx.at[2], self.sx.at[3]
        self.cy = p.copy(two, self.ry, send.at[3], recv.at[3], "y")
        self.cza = p.copy(one, self.ra, send.at[4], recv.at[4], "za")
        self.czb = p.copy(last, self.rb, send.at[5], recv.at[5], "zb")
        self.at = 2 * p.y + p.za
        mine = self.fin.at[self.at]
        self.back = p.copy(mine, mine, send.at[6], recv.at[6], "za")
        half = self.fin.at[pl.ds(2 * p.y, 2)]
        self.wide = p.copy(half, half, send.at[7], recv.at[7], "y")
        self.done = pltpu.make_async_copy(self.fin, out, self.local.at[0])

    def loads(self):
        p = self.p
        return [
            pltpu.make_async_copy(self.term.at[pl.ds(4 * (2 * x + p.c), 4)], to, self.local.at[k])
            for k, (x, to) in enumerate(((1 - p.x, self.sx), (p.x, self.fin)))
        ]

    def a(self):
        for one in self.ka + self.loads():
            one.start()

    def b(self):
        p = self.p
        for one in self.ka:
            one.wait_recv()
        for one in self.loads():
            one.wait()
        for q in range(4):
            self.sx[q] = (self.sx[q].astype(F32) + self.rc[1 - p.x, q].astype(F32)).astype(BF16)
        self.cx.start()
        for q in range(4):
            self.keep[q] = self.fin[q].astype(F32) + self.rc[p.x, q].astype(F32)

    def c_(self):
        self.cx.wait()
        p = self.p
        for q in range(2):
            at = 2 * (1 - p.y) + q
            self.sx[q] = (self.keep[at] + self.rx[at].astype(F32)).astype(BF16)
        self.cy.start()
        for q in range(2):
            at = 2 * p.y + q
            self.keep[at] = self.keep[at] + self.rx[at].astype(F32)

    def d(self):
        self.cy.wait_recv()
        p = self.p
        self.sx[2] = (self.keep[2 * p.y + 1 - p.za] + self.ry[1 - p.za].astype(F32)).astype(BF16)
        self.cza.start()
        self.keep[self.at] = self.keep[self.at] + self.ry[p.za].astype(F32)

    def e(self):
        self.cza.wait_recv()
        self.sx[3] = (self.keep[self.at] + self.ra[...].astype(F32)).astype(BF16)
        self.czb.start()

    def f(self):
        self.czb.wait_recv()
        piece = (self.sx[3].astype(F32) + self.rb[...].astype(F32)).astype(BF16)
        self.fin[self.at] = piece
        self.back.start()
        wide = piece.astype(F32)
        self.squares[0, 0] += jnp.sum(wide * wide)

    def g(self):
        self.back.wait_recv()
        self.wide.start()

    def h(self):
        self.wide.wait_recv()
        self.done.start()

    def finish(self):
        for one in self.ka + [self.cy, self.cza, self.czb, self.back, self.wide]:
            one.wait_send()
        self.done.wait()


def quarters(shape):
    return (16, shape[0] // 16, shape[1])


def sum_scratch(shape):
    _, a, b = shape
    return [
        pltpu.VMEM((2, 4, a, b), BF16),
        pltpu.VMEM((4, a, b), BF16),
        pltpu.VMEM((4, a, b), BF16),
        pltpu.VMEM((4, a, b), F32),
        pltpu.VMEM((2, a, b), BF16),
        pltpu.VMEM((a, b), BF16),
        pltpu.VMEM((a, b), BF16),
        pltpu.VMEM((4, a, b), BF16),
    ]


def kept_out(shape):
    return sds((4,) + shape[1:], BF16)


def split_up(at, per, refs, count=3):
    return [refs[at + k * per : at + (k + 1) * per] for k in range(count)]


def make_sums(place, terms, outs, squares, own, sems):
    send, recv, local = sems
    return [
        Sum(
            place,
            terms[k],
            outs[k],
            squares,
            own[k],
            (send.at[k], recv.at[k], local.at[k]),
        )
        for k in range(len(terms))
    ]


NEAR = ("c", "x", "y", "za", "zb")


def algebra(g, u, dz):
    sig, act = silu_parts(g)
    z = (act * u).astype(BF16)
    dz = dz.astype(BF16).astype(F32)
    du = (dz * act).astype(BF16)
    dg = (dz * u * (sig + act * (1.0 - sig))).astype(BF16)
    return z, dg, du


def store_turned(out, acc):
    n = out.shape[1]
    for at in range(0, acc.shape[1], 128):
        block = acc[:, at : at + 128].T.astype(BF16)
        row = at
        while row < at + 128:
            k, r = row // n, row % n
            more = min(n - r, at + 128 - row)
            out[k, r : r + more, :] = block[row - at : row - at + more, :]
            row += more


def store_quarters(out, acc):
    n = out.shape[1]
    for k in range(out.shape[0]):
        out[k] = acc[k * n : (k + 1) * n, :].astype(BF16)


def hidden_body(a_ref, dy_ref, across_ref, wg_ref, wu_ref, wd_ref, dg_ref, du_ref, dwg_ref, dwu_ref, dwd_ref, acc_g, acc_u, acc_d):
    i = pl.program_id(0)

    @pl.when(i == 0)
    def _():
        for acc in (acc_g, acc_u, acc_d):
            acc[...] = jnp.zeros_like(acc)

    a, dy, across_a = a_ref[...], dy_ref[...], across_ref[...]
    across = dy.T
    for at, n in cuts(acc_d.shape[1]):
        at = slice(at, at + n)
        g, u = dot(a, wg_ref[:, at]), dot(a, wu_ref[:, at])
        z, dg, du = algebra(g, u, dot(dy, wd_ref[at, :], 1, 1))
        dg_ref[:, at] = dg
        du_ref[:, at] = du
        acc_d[:, at] += dot(across, z)
        acc_g[:, at] += dot(across_a, dg)
        acc_u[:, at] += dot(across_a, du)

    @pl.when(i == pl.num_programs(0) - 1)
    def _():
        store_quarters(dwg_ref, acc_g)
        store_quarters(dwu_ref, acc_u)
        store_turned(dwd_ref, acc_d)


def hidden(a, dy, across, wg, wu, wd):
    t, d = dy.shape
    f = wd.shape[0]
    tile = HIDDEN_TILE
    shapes = [quarters((d, f)), quarters((d, f)), quarters((f, d))]
    return pl.pallas_call(
        hidden_body,
        grid=(t // tile,),
        in_specs=[rows(tile, d), rows(tile, d), columns(d, tile), once(d, f), once(d, f), once(f, d)],
        out_specs=[rows(tile, f), rows(tile, f)] + [once(*one) for one in shapes],
        out_shape=[sds((t, f), BF16), sds((t, f), BF16)] + [sds(one, BF16) for one in shapes],
        scratch_shapes=[pltpu.VMEM((d, f), F32)] * 3,
        compiler_params=pltpu.CompilerParams(dimension_semantics=("arbitrary",), vmem_limit_bytes=67043328),
        cost_estimate=cost(12 * t * d * f, 12 * t * f),
        name="hidden",
    )(a, dy, across, wg, wu, wd)


def back_body(dg1, du1, h_ref, dy_ref, g_ref, u_ref, wg_ref, wu_ref, wd_ref, *refs):
    terms, refs = refs[:3], refs[3:]
    dg_ref, du_ref, dwd_ref, sq_ref = refs[:4]
    outs, acc, own, sems = refs[4:7], refs[7], split_up(8, 8, refs), refs[32:]
    i = pl.program_id(0)
    place = Place()
    sums = make_sums(place, terms, outs, sq_ref, own, sems)

    @pl.when(i == 0)
    def _():
        place.greet(NEAR)
        sq_ref[0, 0] = 0.0
        for k in (2, 0, 1):
            sums[k].a()
        acc[...] = jnp.zeros_like(acc)

    plan = {1: ("b2",), 2: ("b0",), 3: ("b1",), 5: ("c2",), 7: ("d2", "c0"), 8: ("e2",), 9: ("d0", "f2"), 10: ("c1", "e0"), 11: ("g2", "f0"), 12: ("d1",), 13: ("h2", "g0", "e1"), 14: ("f1",), 15: ("h0", "g1")}
    for at, what in plan.items():

        @pl.when(i == at)
        def _(what=what):
            for one in what:
                stage(sums, one)

    da = dot(dg1[...], wg_ref[...], 1, 1) + dot(du1[...], wu_ref[...], 1, 1)
    da = da.astype(BF16).astype(F32)
    h = h_ref[...].astype(F32)
    count = h.shape[-1]
    scale = lax.rsqrt(jnp.sum(h * h, -1, keepdims=True) / count + 1e-6)
    inner = jnp.sum(da * h, -1, keepdims=True) / count
    dh = da * scale - h * (inner * (scale * scale * scale))
    dh = (dy_ref[...].astype(F32) + dh.astype(BF16).astype(F32)).astype(BF16)
    across = dh.T
    for at, n in cuts(acc.shape[1]):
        at = slice(at, at + n)
        z, dg, du = algebra(g_ref[:, at], u_ref[:, at], dot(dh, wd_ref[at, :], 1, 1))
        dg_ref[:, at] = dg
        du_ref[:, at] = du
        acc[:, at] += dot(across, z)

    @pl.when(i == pl.num_programs(0) - 1)
    def _():
        store_turned(dwd_ref, acc)
        stage(sums, "h1")
        for one in sums:
            one.finish()


def stage(sums, what):
    one = sums[int(what[1])]
    {"a": one.a, "b": one.b, "c": one.c_, "d": one.d, "e": one.e, "f": one.f, "g": one.g, "h": one.h}[what[0]]()


def sum_outs(shapes):
    return [kept_out(one) for one in shapes]


def sum_own(shapes):
    out = []
    for one in shapes:
        out += sum_scratch(one)
    n = len(shapes)
    return out + [DMA((n, 8)), DMA((n, 8)), DMA((n, 4))]


def back(dg1, du1, h, dy, g0, u0, wg, wu, wd, terms):
    t, d = h.shape
    f = wd.shape[0]
    tile = 256
    shapes = [one.shape for one in terms]
    out = quarters((f, d))
    kinds = sum_outs(shapes)
    results = pl.pallas_call(
        back_body,
        grid=(t // tile,),
        in_specs=[rows(tile, f), rows(tile, f), rows(tile, d), rows(tile, d), rows(tile, f), rows(tile, f)]
        + [once(d, f), once(d, f), once(f, d)]
        + [ANY] * 3,
        out_specs=[rows(tile, f), rows(tile, f), once(*out), pl.BlockSpec(memory_space=pltpu.SMEM)] + [ANY] * len(kinds),
        out_shape=[sds((t, f), BF16), sds((t, f), BF16), sds(out, BF16), sds((1, 1), F32)] + kinds,
        scratch_shapes=[pltpu.VMEM((d, f), F32)] + sum_own(shapes),
        compiler_params=pltpu.CompilerParams(
            dimension_semantics=("arbitrary",), vmem_limit_bytes=67043328, collective_id=1, has_side_effects=True
        ),
        cost_estimate=cost(8 * t * d * f, 12 * t * f),
        name="back",
    )(dg1, du1, h, dy, g0, u0, wg, wu, wd, *terms)
    return results[:3], results[3], results[4:7]


def tail_body(a_ref, c_ref, e_ref, term_d, sq1_ref, *refs):
    tot_ref, g_ref, u_ref, d_ref = refs[:4]
    refs = refs[4:]
    sq_ref, acc, made, own, refs = refs[0], refs[1], refs[2:5], split_up(5, 8, refs, 4), refs[37:]
    terms = (*made, term_d)
    tot_in, tot_send, tot_recv = refs[3:6]
    i = pl.program_id(0)
    n = pl.num_programs(0) // 3
    cut = made[1].shape[2]
    outs = (g_ref, u_ref.at[:, :, pl.ds(0, cut)], u_ref.at[:, :, pl.ds(cut, u_ref.shape[2] - cut)], d_ref)
    place = Place()
    sums = make_sums(place, terms, outs, sq_ref, own, refs[:3])

    @pl.when(i == 0)
    def _():
        place.greet(NEAR)
        sq_ref[0, 0] = sq1_ref[0, 0]
        sums[3].a()

    @pl.when((i == 0) | (i == n))
    def _():
        acc[...] = jnp.zeros_like(acc)

    plan = {1: ("b3",), 5: ("b0", "c3"), 7: ("d3",), 8: ("e3",), 9: ("b1", "c0"), 10: ("f3", "d0"), 11: ("g3",)}
    for at, what in plan.items():

        @pl.when(i == at)
        def _(what=what):
            for one in what:
                stage(sums, one)

    def add(ref, lo, hi):
        across = a_ref[...]
        for at in range(lo, hi, 256):
            at = slice(at, min(at + 256, hi))
            acc[:, at] += dot(across, ref[:, at])

    for k, (ref, lo, hi) in enumerate(((c_ref, 0, c_ref.shape[1]), (e_ref, 0, cut), (e_ref, cut, c_ref.shape[1]))):

        @pl.when((i >= k * n) & (i < (k + 1) * n))
        def _(ref=ref, lo=lo, hi=hi):
            add(ref, lo, hi)

        @pl.when(i == (k + 1) * n - 1)
        def _(k=k, lo=lo, hi=hi):
            rows_each = made[k].shape[1]
            for q in range(16):
                made[k][q] = acc[q * rows_each : (q + 1) * rows_each, lo:hi].astype(BF16)
            sums[k].a()

    @pl.when(i == pl.num_programs(0) - 1)
    def _():
        for one in ("b2", "e0", "c1", "h3", "f0", "d1", "c2", "g0", "e1", "d2", "f1", "e2", "g1", "f2"):
            stage(sums, one)
        tot_ref[...] = jnp.full(tot_ref.shape, sq_ref[0, 0], F32)
        for k, name in enumerate(("c", "x", "y", "za")):
            if k == 1:
                sums[2].g()
            one = place.copy(tot_ref, tot_in.at[k], tot_send.at[k], tot_recv.at[k], name)
            one.start()
            one.wait()
            tot_ref[...] = tot_ref[...] + tot_in[k]
        for one in ("h0", "h1", "h2"):
            stage(sums, one)
        for one in sums:
            one.finish()


def tail(a, c, e, term_d, squares):
    (d, t), f = a.shape, c.shape[1]
    tile = 1024
    n = t // tile
    cut = f // 256 // 2 * 256 + 256
    made = quarters((d, f))
    shapes = [made, made[:2] + (cut,), made[:2] + (f - cut,), term_d.shape]
    kinds = sum_outs([made, made, term_d.shape])
    smem = pl.BlockSpec(memory_space=pltpu.SMEM)
    results = pl.pallas_call(
        tail_body,
        grid=(3 * n,),
        in_specs=[
            pl.BlockSpec((d, tile), lambda i: (0, i % n)),
            pl.BlockSpec((tile, f), lambda i: (jnp.minimum(i, n - 1), 0)),
            pl.BlockSpec((tile, f), lambda i: (jnp.where(i < n, 0, i % n), 0)),
            ANY,
            smem,
        ],
        out_specs=[pl.BlockSpec((8, 128), lambda i: (0, 0))] + [ANY] * len(kinds),
        out_shape=[sds((8, 128), F32)] + kinds,
        scratch_shapes=[pltpu.SMEM((1, 1), F32), pltpu.VMEM((d, f), F32)]
        + [pltpu.VMEM(one, BF16) for one in shapes[:3]]
        + sum_own(shapes)
        + [pltpu.VMEM((4, 8, 128), F32), DMA((4,)), DMA((4,))],
        compiler_params=pltpu.CompilerParams(
            dimension_semantics=("arbitrary",), vmem_limit_bytes=67043328, collective_id=2, has_side_effects=True
        ),
        cost_estimate=cost(4 * t * d * f, 4 * t * f),
        name="tail",
    )(a, c, e, term_d, squares)
    return results[0][0, 0], results[1:4]


def solution(mesh):
    def step(x, dy, *arrays):
        x, dy = x[0], dy[0]
        weights, m, v = (arrays[i : i + 3] for i in (0, 3, 6))
        g0, u0, h1, a1, across0, across1, wd0, wg1, wu1, wd1 = forward(x, *weights)
        dg1, du1, d_wg1, d_wu1, d_wd1 = hidden(a1, dy, across1, wg1, wu1, wd1)
        (dg0, du0, d_wd0), squares1, sums1 = back(dg1, du1, h1, dy, g0, u0, wg1, wu1, wd0, (d_wg1, d_wu1, d_wd1))
        squares, sums0 = tail(across0, dg0, du0, d_wd0, squares1)
        count = 4 * sum(w.size for w in weights)
        factor = jnp.minimum(1.0, 0.5 * lax.rsqrt(squares / count + 1e-30))
        new = []
        for i in range(3):
            g = jnp.stack([sums0[i], sums1[i]]).reshape(weights[i].shape).astype(F32) * factor
            w = weights[i].astype(F32)
            mi = 0.9 * m[i] + 0.1 * g
            vi = 0.95 * v[i] + 0.05 * g * g
            new.append(((w - 0.02 * (mi * lax.rsqrt(vi + 1e-8) + 0.1 * w)).astype(BF16), mi, vi))
        return tuple(one[which] for which in range(3) for one in new)

    states, cut = P(("rep", "r", "s"), None, None), P(None, "s", None)
    return jax.shard_map(
        step,
        mesh=mesh,
        in_specs=(states, states) + (cut,) * 9,
        out_specs=(P("rep", "s", None),) * 9,
        check_vma=False,
    )
```
